32 devices in a mesh: paper: 8 (over z, y), author: 4 (over x, core).
Axes of the slice: x: 2, y: 2, z: 4, core: 2. Of those that a mesh axis runs over, the one named last changes fastest.
Arguments:
- paper_feat: bfloat16 [2048, 1024], P('paper', 'author'), may hold values from -6 to 6
- author_feat: bfloat16 [2048, 1024], P('paper', 'author'), may hold values from -6 to 6
- cite_owner: int32 [384, 1], P('paper'), may hold values from 0 to 7; in each aligned block of 48 rows (0 to 47, 48 to 95, ...) at most 7 rows name the same one
- cite_source: int32 [384], P('paper'), may hold values from 0 to 1
- cite_target: int32 [384], P('paper'), may hold values from 0 to 1
- cite_edges: int32 [384], P('paper'), may hold values from 8 to 64
- cite_count: int32 [8], P('paper'), may hold values from 36 to 48, as said below
- citation_weight_tiles: bfloat16 [384, 128, 128], P('paper'), may hold values from 0 to 1
- write_owner: int32 [256, 1], P('paper'), may hold values from 0 to 7; in each aligned block of 32 rows (0 to 31, 32 to 63, ...) at most 5 rows name the same one
- write_paper: int32 [256], P('paper'), may hold values from 0 to 1
- write_author: int32 [256], P('paper'), may hold values from 0 to 1
- write_edges: int32 [256], P('paper'), may hold values from 8 to 64
- authorship_weight_tiles: bfloat16 [256, 128, 128], P('paper'), may hold values from 0 to 1
- w_self: bfloat16 [1024, 1024], replicated, may hold values from -0.1875 to 0.1875
- w_cite: bfloat16 [1024, 1024], replicated, may hold values from -0.1875 to 0.1875
- w_write: bfloat16 [1024, 1024], replicated, may hold values from -0.1875 to 0.1875
- cotangent: bfloat16 [2048, 1024], P('paper', 'author'), may hold values from -6 to 6
Outputs:
- paper_out: bfloat16 [2048, 1024], P('paper', 'author')
- paper_grad: bfloat16 [2048, 1024], P('paper', 'author')
- author_grad: bfloat16 [2048, 1024], P('paper', 'author')
The draws below stay inside these ranges and needn't reach their ends.
Inputs may be any that keep to these rules, and one draw needn't show every extreme that they name: `cite_owner`: among the 48 tiles of one paper index (live or not), at most 7 have their source on any one paper index. The live tiles of a paper index are the first cite_count of its list; some paper index has all 48 live. `write_owner`: among the 32 tiles of one paper index, at most 5 take their author block from any one paper index.
All inputs are finite; a program needn't handle non-finite values.
Results may differ from the reference program's by a relative error of at most 0.007.
Values may be sent and summed in bfloat16 or wider, within the bound.
No kernel may reach another device: no remote copies, remote signals or barrier semaphores. Data moves between devices by JAX's collectives and lax.ppermute only.
A program may use at most 128 MiB of HBM per device.

```python
import math
import jax
import jax.numpy as jnp
import numpy as np
from jax import lax

D = 1024
BLOCK = 128
P_BLOCKS = 2
A_BLOCKS = 2
CITE_TILES = 48
WRITE_TILES = 32
SLOTS = 7
WSLOTS = 5
PAPERS = 2048
AUTHORS = 2048
N_PAPER = 8


def draw_cite_count(key, part):
    key = jax.random.fold_in(key, 11)
    first_key, second_key = jax.random.split(key)
    missing = jax.random.randint(first_key, (N_PAPER,), 0, CITE_TILES // 4 + 1)
    counts = CITE_TILES - missing
    chosen = jax.random.randint(second_key, (), 0, N_PAPER)
    return jnp.where(jnp.arange(N_PAPER) == chosen, CITE_TILES, counts).astype(jnp.int32)


def place_ends(result, key, smallest, largest):
    index_at = [jax.random.randint(jax.random.fold_in(key, axis), (), 0, length) for axis, length in enumerate(result.shape)]
    main_axis = result.shape.index(max(result.shape))
    next_to = index_at[:main_axis] + [(index_at[main_axis] + 1) % result.shape[main_axis]] + index_at[main_axis + 1:]
    return result.at[tuple(index_at)].set(smallest).at[tuple(next_to)].set(largest)


def steps_of(rng, extent, pieces, smallest, largest):
    loudness = 1.0
    for dim, parts in pieces:
        steps = jax.random.uniform(jax.random.fold_in(jax.random.fold_in(rng, 6), dim), (parts,), jnp.float32, smallest / len(pieces), largest / len(pieces))
        loudness = loudness * jnp.repeat(jnp.exp(steps), extent[dim] // parts).reshape((-1,) + (1,) * (len(extent) - 1 - dim))
    return loudness


def routed_block(own_key, own, number, rows, count, top, limit, slope):
    ranking = jax.random.permutation(own_key, count)
    packed, usual = shares(count, rows * top, limit, slope, True), shares(count, rows * top, limit, slope, False)
    places = jnp.arange(count)

    def named(tallies, turn):
        used = int((tallies > 0).sum())
        fixed = max(1, used // 4)
        passed = fixed + (places - fixed + turn * (used - fixed)) % max(1, count - fixed)
        return jnp.zeros((count,), jnp.int32).at[ranking[jnp.where(places < fixed, places, passed)]].set(jnp.asarray(tallies, jnp.int32))

    tallies = jnp.where(number % 4 == 0, named(packed, number // 4), named(usual, number - number // 4 - 1))
    mixed = jax.random.permutation(jax.random.fold_in(own, 3), count)
    source_of, sink = mixed[0:count // 2 * 2:2], mixed[1:count // 2 * 2:2]
    slack = jnp.minimum(tallies[source_of] - 1, limit - tallies[sink]) // 2
    slack = jnp.where((source_of == ranking[0]) | (sink == ranking[0]) | (tallies[sink] == 0), 0, jnp.maximum(slack, 0))
    passed = jax.random.randint(jax.random.fold_in(own, 4), (count // 2,), 0, 1 << 20) % (slack + 1)
    tallies = tallies.at[source_of].add(-passed).at[sink].add(passed)
    labels = jnp.searchsorted(jnp.cumsum(tallies), jnp.arange(rows * top), side="right").astype(jnp.int32)
    listing = labels.reshape(top, rows).T
    listing = listing[jax.random.permutation(jax.random.fold_in(own, 1), rows)]
    turn = jax.random.randint(jax.random.fold_in(own, 2), (rows, 1), 0, top)
    return jnp.take_along_axis(listing, (jnp.arange(top)[None, :] + turn) % top, axis=1)


def shares(amount, total, most, lean, full):
    loads = [(1 << 20) // math.isqrt(grade ** lean) + 1 for grade in range(1, amount + 1)]
    largest = most if full else min(most, max(-(-total // amount), total * loads[0] // sum(loads)))
    least = 1 if total - largest >= amount - 1 else 0
    given, rest = [largest] + [least] * (amount - 1), total - largest - least * (amount - 1)
    while rest > 0:
        candidates = [i for i in range(1, amount) if given[i] < largest] or [i for i in range(1, amount) if given[i] < most]
        mass, budget = sum([loads[i] for i in candidates]), rest
        for i in candidates:
            addition = min(most - given[i], max(1, budget * loads[i] // mass), rest)
            given[i] = given[i] + addition
            rest = rest - addition
    return np.array(given)


def centred(key, shape, scale, most, cuts=(), held_as=jnp.bfloat16):
    drawn = scale * jax.random.normal(key, shape, jnp.float32)
    if cuts:
        drawn = drawn * steps_of(key, shape, cuts, -0.22, 0.18)
    return jnp.clip(drawn, -most, most).astype(held_as)


def setup_inputs(seed: int = 0) -> dict:
    key_of = jax.random.split(jax.random.key(seed), 18)
    paper_feat = centred(key_of[0], (PAPERS, D), 1.0, 6.0, ((0, 8), (1, 4)))
    author_feat = centred(key_of[1], (AUTHORS, D), 1.0, 6.0, ((0, 8), (1, 4)))
    cite_owner_keys = jax.random.split(jax.random.fold_in(key_of[2], 1), (N_PAPER * CITE_TILES) // CITE_TILES)
    cite_owner_turns = jax.random.permutation(jax.random.fold_in(key_of[2], 3), (N_PAPER * CITE_TILES) // CITE_TILES)
    cite_owner = jax.vmap(lambda own, number: routed_block(jax.random.fold_in(key_of[2], 2), own, number, CITE_TILES, N_PAPER, 1, SLOTS, 2))(cite_owner_keys, cite_owner_turns).reshape((N_PAPER * CITE_TILES, 1))
    cite_source = place_ends(jax.random.randint(key_of[3], (N_PAPER * CITE_TILES,), 0, P_BLOCKS), jax.random.fold_in(key_of[3], 1), 0, P_BLOCKS - 1).astype(jnp.int32)
    cite_target = place_ends(jax.random.randint(key_of[4], (N_PAPER * CITE_TILES,), 0, P_BLOCKS), jax.random.fold_in(key_of[4], 1), 0, P_BLOCKS - 1).astype(jnp.int32)
    cite_edges = place_ends(jax.random.randint(key_of[5], (N_PAPER * CITE_TILES,), 8, 65), jax.random.fold_in(key_of[5], 1), 8, 64).astype(jnp.int32)
    cite_count = draw_cite_count(jax.random.fold_in(key_of[17], 71), 0)
    citation_weight_tiles = jnp.clip(1.0 * jax.random.uniform(key_of[7], (N_PAPER * CITE_TILES, BLOCK, BLOCK), jnp.float32) ** steps_of(key_of[7], (N_PAPER * CITE_TILES, BLOCK, BLOCK), ((0, 8),), -0.2, 0.2), 0.0, 1.0).astype(jnp.bfloat16)
    write_owner_keys = jax.random.split(jax.random.fold_in(key_of[8], 1), (N_PAPER * WRITE_TILES) // WRITE_TILES)
    write_owner_turns = jax.random.permutation(jax.random.fold_in(key_of[8], 3), (N_PAPER * WRITE_TILES) // WRITE_TILES)
    write_owner = jax.vmap(lambda own, number: routed_block(jax.random.fold_in(key_of[8], 2), own, number, WRITE_TILES, N_PAPER, 1, WSLOTS, 2))(write_owner_keys, write_owner_turns).reshape((N_PAPER * WRITE_TILES, 1))
    write_paper = place_ends(jax.random.randint(key_of[9], (N_PAPER * WRITE_TILES,), 0, P_BLOCKS), jax.random.fold_in(key_of[9], 1), 0, P_BLOCKS - 1).astype(jnp.int32)
    write_author = place_ends(jax.random.randint(key_of[10], (N_PAPER * WRITE_TILES,), 0, A_BLOCKS), jax.random.fold_in(key_of[10], 1), 0, A_BLOCKS - 1).astype(jnp.int32)
    write_edges = place_ends(jax.random.randint(key_of[11], (N_PAPER * WRITE_TILES,), 8, 65), jax.random.fold_in(key_of[11], 1), 8, 64).astype(jnp.int32)
    authorship_weight_tiles = jnp.clip(1.0 * jax.random.uniform(key_of[12], (N_PAPER * WRITE_TILES, BLOCK, BLOCK), jnp.float32) ** steps_of(key_of[12], (N_PAPER * WRITE_TILES, BLOCK, BLOCK), ((0, 8),), -0.2, 0.2), 0.0, 1.0).astype(jnp.bfloat16)
    w_self = centred(key_of[13], (D, D), D ** -0.5, 0.1875)
    w_cite = centred(key_of[14], (D, D), D ** -0.5, 0.1875)
    w_write = centred(key_of[15], (D, D), D ** -0.5, 0.1875)
    cotangent = centred(key_of[16], (PAPERS, D), 1.0, 6.0, ((0, 8), (1, 4)))
    return {"paper_feat": paper_feat, "author_feat": author_feat, "cite_owner": cite_owner, "cite_source": cite_source, "cite_target": cite_target, "cite_edges": cite_edges, "cite_count": cite_count, "citation_weight_tiles": citation_weight_tiles, "write_owner": write_owner, "write_paper": write_paper, "write_author": write_author, "write_edges": write_edges, "authorship_weight_tiles": authorship_weight_tiles, "w_self": w_self, "w_cite": w_cite, "w_write": w_write, "cotangent": cotangent}


TOP_PRECISION = lax.Precision.HIGHEST


def silu_slope(values):
    sigma = jax.nn.sigmoid(values)
    return sigma * (1.0 + values * (1.0 - sigma))


def matmul(left, right):
    return jnp.dot(left, right, preferred_element_type=jnp.float32)


def reference(paper_feat, author_feat, cite_owner, cite_source, cite_target, cite_edges, cite_count, citation_weight_tiles, write_owner, write_paper, write_author, write_edges, authorship_weight_tiles, w_self, w_cite, w_write, cotangent):
    paper_stack = paper_feat.reshape(N_PAPER * P_BLOCKS, BLOCK, D)
    author_stack = author_feat.reshape(N_PAPER * A_BLOCKS, BLOCK, D)
    tile_order = jnp.arange(CITE_TILES, dtype=jnp.int32)
    block_ids = jnp.arange(P_BLOCKS, dtype=jnp.int32)
    live_tile = tile_order[None, :] < cite_count[:, None]
    cite_scale = jnp.where(live_tile, 1.0 / cite_edges.reshape(N_PAPER, CITE_TILES).astype(jnp.float32), jnp.float32(0.0))
    glob_source = (cite_owner[:, 0] * P_BLOCKS + cite_source).astype(jnp.int32).reshape(N_PAPER, CITE_TILES)
    target_group = cite_target.reshape(N_PAPER, CITE_TILES)
    tiles_group = citation_weight_tiles.reshape(N_PAPER, CITE_TILES, BLOCK, BLOCK)

    def cite_group(inputs):
        sources, target_indices, scales, weight_tiles = inputs
        collected_rows = jnp.take(paper_stack, sources, axis=0).astype(jnp.float32)
        block_products = jnp.einsum("eih,ehp->eip", weight_tiles.astype(jnp.float32), collected_rows, precision=TOP_PRECISION)
        edge_weights = jnp.where(target_indices[:, None] == block_ids[None, :], scales[:, None], jnp.float32(0.0))
        return jnp.einsum("nr,nmh->rmh", edge_weights, block_products, precision=TOP_PRECISION)

    cite_sum = lax.map(cite_group, (glob_source, target_group, cite_scale, tiles_group))
    cite_sum = cite_sum.reshape(PAPERS, D).astype(jnp.bfloat16)

    write_glob = (write_owner[:, 0] * A_BLOCKS + write_author).astype(jnp.int32).reshape(N_PAPER, WRITE_TILES)
    write_scale = (1.0 / write_edges.astype(jnp.float32)).reshape(N_PAPER, WRITE_TILES)
    write_target = write_paper.reshape(N_PAPER, WRITE_TILES)
    write_group_tiles = authorship_weight_tiles.reshape(N_PAPER, WRITE_TILES, BLOCK, BLOCK)

    def write_group(inputs):
        sources, target_indices, scales, weight_tiles = inputs
        collected_rows = jnp.take(author_stack, sources, axis=0).astype(jnp.float32)
        block_products = jnp.einsum("eih,ehp->eip", weight_tiles.astype(jnp.float32), collected_rows, precision=TOP_PRECISION)
        edge_weights = jnp.where(target_indices[:, None] == block_ids[None, :], scales[:, None], jnp.float32(0.0))
        return jnp.einsum("nr,nmh->rmh", edge_weights, block_products, precision=TOP_PRECISION)

    authorship_sum = lax.map(write_group, (write_glob, write_target, write_scale, write_group_tiles))
    authorship_sum = authorship_sum.reshape(PAPERS, D).astype(jnp.bfloat16)

    preact = matmul(paper_feat, w_self) + matmul(cite_sum, w_cite) + matmul(authorship_sum, w_write)
    paper_out = (paper_feat.astype(jnp.float32) + jax.nn.silu(preact)).astype(jnp.bfloat16)
    grad_pre = (cotangent.astype(jnp.float32) * silu_slope(preact)).astype(jnp.bfloat16)
    self_back = matmul(grad_pre, w_self.T)
    cite_grad = matmul(grad_pre, w_cite.T).astype(jnp.bfloat16)
    write_grad = matmul(grad_pre, w_write.T).astype(jnp.bfloat16)

    cite_grad_stack = cite_grad.reshape(N_PAPER, P_BLOCKS, BLOCK, D)

    def cite_back_step(total, inputs):
        sources, grads, target_indices, scales, weight_tiles = inputs
        selected_rows = jnp.take(grads, target_indices, axis=0).astype(jnp.float32)
        backward_pass = jnp.einsum("pdg,pdw->pgw", weight_tiles.astype(jnp.float32), selected_rows, precision=TOP_PRECISION)
        backward_pass = (backward_pass * scales[:, None, None]).astype(jnp.bfloat16)
        return total.at[sources].add(backward_pass.astype(jnp.float32)), None

    returned, _ = lax.scan(cite_back_step, jnp.zeros((N_PAPER * P_BLOCKS, BLOCK, D), jnp.float32), (glob_source, cite_grad_stack, target_group, cite_scale, tiles_group))
    paper_grad = (cotangent.astype(jnp.float32) + self_back + returned.reshape(PAPERS, D)).astype(jnp.bfloat16)

    write_grad_stack = write_grad.reshape(N_PAPER, P_BLOCKS, BLOCK, D)

    def author_back_step(total, inputs):
        sources, grads, target_indices, scales, weight_tiles = inputs
        selected_rows = jnp.take(grads, target_indices, axis=0).astype(jnp.float32)
        backward_pass = jnp.einsum("pdg,pdw->pgw", weight_tiles.astype(jnp.float32), selected_rows, precision=TOP_PRECISION)
        backward_pass = (backward_pass * scales[:, None, None]).astype(jnp.bfloat16)
        return total.at[sources].add(backward_pass.astype(jnp.float32)), None

    author_total, _ = lax.scan(author_back_step, jnp.zeros((N_PAPER * A_BLOCKS, BLOCK, D), jnp.float32), (write_glob, write_grad_stack, write_target, write_scale, write_group_tiles))
    author_grad = author_total.reshape(AUTHORS, D).astype(jnp.bfloat16)
    return paper_out, paper_grad, author_grad
```

```python
import jax
import jax.numpy as jnp
from jax import lax
from jax.experimental import pallas as pl
from jax.experimental.pallas import tpu as pltpu
from jax.sharding import PartitionSpec as P


def silu_slope(values):
    sigma = jax.nn.sigmoid(values)
    return sigma * (1.0 + values * (1.0 - sigma))


def matmul(left, right):
    return jnp.dot(left, right, preferred_element_type=jnp.float32)


def matmul_flipped(left, right):
    return lax.dot_general(
        left, right, (((1,), (1,)), ((), ())), preferred_element_type=jnp.float32
    )


def matmul_rows(left, right):
    return lax.dot_general(
        left, right, (((0,), (0,)), ((), ())), preferred_element_type=jnp.float32
    )


def ring_order(count):
    if count % 2:
        return list(range(count))
    return list(range(0, count, 2)) + list(range(count - 1, 0, -2))


def ring_place(index, count):
    if count % 2:
        return index
    return jnp.where(index % 2 == 0, index // 2, count - (index + 1) // 2)


def ring_pairs(count, step):
    order = ring_order(count)
    return [(order[i], order[(i + step) % count]) for i in range(count)]


def ring_gather(block, count, first):
    ups = count // 2 if first > 0 else (count - 1) // 2
    blocks = {0: block}
    held = block
    for step in range(1, ups + 1):
        held = lax.ppermute(held, "paper", ring_pairs(count, 1))
        blocks[count - step] = held
    held = block
    for step in range(1, count - ups):
        held = lax.ppermute(held, "paper", ring_pairs(count, -1))
        blocks[step] = held
    return [blocks[i] for i in range(count)]


def ring_scatter(partial, count, first):
    ups = count // 2 if first > 0 else (count - 1) // 2
    total = partial(0)
    for reach, step in ((ups, 1), (count - 1 - ups, -1)):
        if reach == 0:
            continue
        held = partial(reach * step % count).astype(jnp.bfloat16)
        for place in range(reach - 1, 0, -1):
            held = lax.ppermute(held, "paper", ring_pairs(count, step)).astype(jnp.float32)
            held = (held + partial(place * step % count)).astype(jnp.bfloat16)
        total = total + lax.ppermute(held, "paper", ring_pairs(count, step)).astype(jnp.float32)
    return total


def feature_gather(part, count):
    parts = {0: part}
    bit = count // 2
    while bit:
        pairs = [(i, i ^ bit) for i in range(count)]
        parts.update({r ^ bit: lax.ppermute(v, "author", pairs) for r, v in list(parts.items())})
        bit //= 2
    return [parts[r] for r in range(count)]


def adjacency_kernel(place_ref, scale_ref, tiles_ref, out_ref, acc_ref):
    groups, rows, cols = out_ref.shape
    side = tiles_ref.shape[1]
    across = cols // side
    down = rows // side
    acc_ref[...] = jnp.zeros(acc_ref.shape, jnp.float32)

    def add(tile, carry):
        place = place_ref[tile]
        acc_ref[place] += scale_ref[tile] * tiles_ref[tile].astype(jnp.float32)
        return carry

    lax.fori_loop(0, tiles_ref.shape[0], add, 0)

    def store(group, carry):
        for i in range(down):
            for j in range(across):
                out_ref[group, i * side:(i + 1) * side, j * side:(j + 1) * side] = acc_ref[
                    (group * down + i) * across + j
                ].astype(jnp.bfloat16)
        return carry

    lax.fori_loop(0, groups, store, 0)


def adjacency(place, scale, tiles, groups, down, across):
    side = tiles.shape[1]
    return pl.pallas_call(
        adjacency_kernel,
        out_shape=jax.ShapeDtypeStruct((groups, down * side, across * side), jnp.bfloat16),
        in_specs=[
            pl.BlockSpec(memory_space=pltpu.SMEM),
            pl.BlockSpec(memory_space=pltpu.SMEM),
            pl.BlockSpec(memory_space=pltpu.VMEM),
        ],
        out_specs=pl.BlockSpec(memory_space=pltpu.VMEM),
        scratch_shapes=[pltpu.VMEM((groups * down * across, side, side), jnp.float32)],
    )(place, scale, tiles)


def body(
    paper_feat,
    author_feat,
    cite_owner,
    cite_source,
    cite_target,
    cite_edges,
    cite_count,
    citation_weight_tiles,
    write_owner,
    write_paper,
    write_author,
    write_edges,
    authorship_weight_tiles,
    w_self,
    w_cite,
    w_write,
    cotangent,
):
    peers = lax.axis_size("paper")
    columns = lax.axis_size("author")
    side = citation_weight_tiles.shape[1]
    paper_rows, quarter = paper_feat.shape
    author_rows = author_feat.shape[0]
    paper_blocks = paper_rows // side
    author_blocks = author_rows // side
    here = ring_place(lax.axis_index("paper"), peers)
    mine = lax.axis_index("author")

    def rel(owner):
        return (ring_place(owner, peers) - here) % peers

    cite_place = (rel(cite_owner[:, 0]) * paper_blocks + cite_target) * paper_blocks + cite_source
    live = jnp.arange(cite_target.shape[0], dtype=jnp.int32) < cite_count[0]
    cite_scale = jnp.where(live, 1.0 / cite_edges.astype(jnp.float32), 0.0)
    write_place = (rel(write_owner[:, 0]) * paper_blocks + write_paper) * author_blocks + write_author
    write_scale = 1.0 / write_edges.astype(jnp.float32)

    authors = ring_gather(author_feat, peers, 1)
    feats = feature_gather(paper_feat, columns)

    write_adj = adjacency(
        write_place, write_scale, authorship_weight_tiles, peers, paper_blocks, author_blocks
    )
    cite_adj = adjacency(
        cite_place, cite_scale, citation_weight_tiles, peers, paper_blocks, paper_blocks
    )

    def project(parts, weight):
        return sum(
            matmul(
                part,
                lax.dynamic_slice(weight, ((mine ^ r) * quarter, mine * quarter), (quarter, quarter)),
            )
            for r, part in enumerate(parts)
        )

    def project_back(parts, weight):
        return sum(
            matmul_flipped(
                part,
                lax.dynamic_slice(weight, (mine * quarter, (mine ^ r) * quarter), (quarter, quarter)),
            )
            for r, part in enumerate(parts)
        )

    projected = ring_gather(project(feats, w_cite).astype(jnp.bfloat16), peers, -1)
    write_sum = sum(matmul(write_adj[i], authors[i]) for i in range(peers)).astype(jnp.bfloat16)
    writes = feature_gather(write_sum, columns)
    preact = project(feats, w_self) + project(writes, w_write)
    preact = preact + sum(matmul(cite_adj[i], projected[i]) for i in range(peers))
    paper_out = (paper_feat.astype(jnp.float32) + jax.nn.silu(preact)).astype(jnp.bfloat16)
    grad_pre = (cotangent.astype(jnp.float32) * silu_slope(preact)).astype(jnp.bfloat16)

    author_sum = ring_scatter(lambda i: matmul_rows(write_adj[i], grad_pre), peers, 1)
    grads = feature_gather(grad_pre, columns)
    cite_grad = project_back(grads, w_cite).astype(jnp.bfloat16)
    cite_return = ring_scatter(lambda i: matmul_rows(cite_adj[i], cite_grad), peers, -1)
    self_back = project_back(grads, w_self)
    paper_grad = (cotangent.astype(jnp.float32) + self_back + cite_return).astype(jnp.bfloat16)
    author_sums = feature_gather(author_sum.astype(jnp.bfloat16), columns)
    author_grad = project_back(author_sums, w_write).astype(jnp.bfloat16)
    return (paper_out, paper_grad, author_grad)


def solution(mesh):
    in_specs = (
        P("paper", "author"),
        P("paper", "author"),
        P("paper", None),
        P("paper"),
        P("paper"),
        P("paper"),
        P("paper"),
        P("paper", None, None),
        P("paper", None),
        P("paper"),
        P("paper"),
        P("paper"),
        P("paper", None, None),
        P(),
        P(),
        P(),
        P("paper", "author"),
    )
    out_specs = (P("paper", "author"), P("paper", "author"), P("paper", "author"))
    return jax.shard_map(body, mesh=mesh, in_specs=in_specs, out_specs=out_specs, check_vma=False)
```

```python
import functools
import jax
import jax.numpy as jnp
from jax import lax
from jax.experimental import pallas as pl
from jax.experimental.pallas import tpu as pltpu
from jax.sharding import PartitionSpec as P


def matmul(left, right):
    return jnp.dot(left, right, preferred_element_type=jnp.float32)


def matmul_flipped(left, right):
    return lax.dot_general(
        left, right, (((1,), (1,)), ((), ())), preferred_element_type=jnp.float32
    )


def matmul_rows(left, right):
    return lax.dot_general(
        left, right, (((0,), (0,)), ((), ())), preferred_element_type=jnp.float32
    )


def ring_order(count):
    if count % 2:
        return list(range(count))
    return list(range(0, count, 2)) + list(range(count - 1, 0, -2))


def ring_place(index, count):
    if count % 2:
        return index
    return jnp.where(index % 2 == 0, index // 2, count - (index + 1) // 2)


def ring_pairs(count, step):
    order = ring_order(count)
    return [(order[i], order[(i + step) % count]) for i in range(count)]


def ring_gather(block, count, first):
    ups = count // 2 if first > 0 else (count - 1) // 2
    blocks = {0: block}
    for reach, step in ((ups, 1), (count - 1 - ups, -1)):
        held = block
        for place in range(1, reach + 1):
            held = lax.ppermute(held, "paper", ring_pairs(count, step))
            blocks[-place * step % count] = held
    return [blocks[i] for i in range(count)]


def ring_scatter(partials, count, first):
    ups = count // 2 if first > 0 else (count - 1) // 2
    total = partials[0]
    for reach, step in ((ups, 1), (count - 1 - ups, -1)):
        if reach == 0:
            continue
        held = partials[reach * step % count]
        for place in range(reach - 1, 0, -1):
            held = lax.ppermute(held, "paper", ring_pairs(count, step))
            held = held.astype(jnp.float32) + partials[place * step % count].astype(jnp.float32)
            held = held.astype(jnp.bfloat16)
        held = lax.ppermute(held, "paper", ring_pairs(count, step))
        total = total + held.astype(jnp.float32)
    return total


def feature_gather(part, count):
    parts = {0: part}
    bit = count // 2
    while bit:
        pairs = [(i, i ^ bit) for i in range(count)]
        for r, held in list(parts.items()):
            parts[r ^ bit] = lax.ppermute(held, "author", pairs)
        bit //= 2
    return [parts[r] for r in range(count)]


VMEM_ELEMENTS = 1 << 20
VMEM_GRANT = 12 << 20
SMEM = pl.BlockSpec(memory_space=pltpu.SMEM)
VMEM = pl.BlockSpec(memory_space=pltpu.VMEM)


def adjacency_kernel(peers, counted, mine_ref, owner_ref, inner_ref, outer_ref, edges_ref, tiles_ref, *refs):
    out_ref, acc_ref = refs[-2:]
    groups, rows, cols = out_ref.shape
    side = tiles_ref.shape[1]
    across = cols // side
    down = rows // side
    here = ring_place(mine_ref[0], peers)
    limit = mine_ref[2] if counted else tiles_ref.shape[0]
    acc_ref[...] = jnp.zeros(acc_ref.shape, jnp.float32)

    def add(tile, carry):
        group = lax.rem(ring_place(owner_ref[tile], peers) - here + peers, peers)
        place = (group * down + inner_ref[tile]) * across + outer_ref[tile]
        edges = jnp.full((1, side), edges_ref[tile].astype(jnp.float32))
        live = jnp.where(tile < limit, 1.0, 0.0)
        acc_ref[place] += (live / edges) * tiles_ref[tile].astype(jnp.float32)
        return carry

    lax.fori_loop(0, tiles_ref.shape[0], add, 0, unroll=2)

    def store(group, carry):
        for i in range(down):
            for j in range(across):
                out_ref[group, i * side:(i + 1) * side, j * side:(j + 1) * side] = acc_ref[
                    (group * down + i) * across + j
                ].astype(jnp.bfloat16)
        return carry

    lax.fori_loop(0, groups, store, 0)


def adjacency(counted, mine, tables, tiles, peers, down, across, near, after):
    side = tiles.shape[1]
    call = pl.pallas_call(
        functools.partial(adjacency_kernel, peers, counted),
        out_shape=(pltpu.VMEM if near else jax.ShapeDtypeStruct)(
            (peers, down * side, across * side), jnp.bfloat16
        ),
        in_specs=[SMEM] * 5 + [VMEM] * (1 + len(after)),
        out_specs=VMEM,
        compiler_params=grant(near),
        scratch_shapes=[pltpu.VMEM((peers * down * across, side, side), jnp.float32)],
    )
    return call(
        mine, *tables, placed(tiles, near), *[placed(v, near) for v in after]
    )


def project_sum(mine, parts, weight_ref):
    quarter = parts[0].shape[1]
    total = None
    for r, part in enumerate(parts):
        start = pl.multiple_of((mine ^ r) * quarter, quarter)
        piece = matmul(part[...], weight_ref[pl.ds(start, quarter), :])
        total = piece if total is None else total + piece
    return total


def project_back_sum(mine, parts, weight_ref):
    quarter = parts[0].shape[1]
    own = pl.multiple_of(mine * quarter, quarter)
    total = None
    for r, part in enumerate(parts):
        start = pl.multiple_of((mine ^ r) * quarter, quarter)
        piece = matmul_flipped(part[...], weight_ref[pl.ds(own, quarter), pl.ds(start, quarter)])
        total = piece if total is None else total + piece
    return total


def fits(rows, cols):
    return rows * cols <= VMEM_ELEMENTS


def grant(near):
    return pltpu.CompilerParams(vmem_limit_bytes=VMEM_GRANT) if near else None


def placed(array, near):
    return pltpu.with_memory_space_constraint(array, pltpu.VMEM) if near else array


def run(kernel, mine, inputs, outs, near, after=(), kept=()):
    return pl.pallas_call(
        kernel,
        in_specs=[SMEM] + [VMEM] * (len(inputs) + len(after)),
        out_specs=[VMEM] * len(outs),
        out_shape=[
            (pltpu.VMEM if near and i not in kept else jax.ShapeDtypeStruct)(shape, dtype)
            for i, (shape, dtype) in enumerate(outs)
        ],
        compiler_params=grant(near),
    )(mine, *[placed(v, near) for v in inputs], *[placed(v, near) for v in after])


def fetch_kernel(weight_count, place_ref, count_ref, *refs):
    scalars_ref, sems = refs[-2:]
    refs = refs[:-2]
    sources, targets = refs[:len(refs) // 2], refs[len(refs) // 2:]
    quarter = targets[0].shape[1]
    own = pl.multiple_of(place_ref[1] * quarter, quarter)
    copies = []
    for i, (source, target) in enumerate(zip(sources, targets)):
        if i < weight_count:
            source = source.at[:, pl.ds(own, quarter)]
        copies.append(pltpu.make_async_copy(source, target, sems.at[i]))
    for copy in copies:
        copy.start()
    scalars_ref[0] = place_ref[0]
    scalars_ref[1] = place_ref[1]
    scalars_ref[2] = count_ref[0]
    for copy in copies:
        copy.wait()


def fetch(places, live, weights, tables, quarter, near):
    space = pltpu.VMEM if near else jax.ShapeDtypeStruct
    sources = [pltpu.with_memory_space_constraint(v, pltpu.HBM) for v in [*weights, *tables]]
    call = pl.pallas_call(
        functools.partial(fetch_kernel, len(weights)),
        in_specs=[SMEM, SMEM] + [pl.BlockSpec(memory_space=pltpu.HBM)] * len(sources),
        out_specs=[VMEM] * len(weights) + [SMEM] * (len(tables) + 1),
        out_shape=[space((weight.shape[0], quarter), weight.dtype) for weight in weights]
        + [pltpu.SMEM(table.shape, jnp.int32) for table in tables]
        + [pltpu.SMEM((3,), jnp.int32)],
        scratch_shapes=[pltpu.SemaphoreType.DMA((len(sources),))],
        compiler_params=grant(near),
    )
    *found, scalars = call(places, live, *sources)
    return found[:len(weights)], found[len(weights):], scalars


def enter_kernel(columns, mine_ref, *refs):
    parts, (cite_ref, self_ref) = refs[:columns], refs[columns:columns + 2]
    projected_ref, kept_ref = refs[-2:]
    mine = mine_ref[1]
    projected_ref[...] = project_sum(mine, parts, cite_ref).astype(jnp.bfloat16)
    kept_ref[...] = project_sum(mine, parts, self_ref)


def gather_kernel(peers, mine_ref, *refs):
    blocks, adj_ref, out_ref = refs[:peers], refs[peers], refs[-1]
    total = matmul(adj_ref[0], blocks[0][...])
    for i in range(1, peers):
        total = total + matmul(adj_ref[i], blocks[i][...])
    out_ref[...] = total.astype(jnp.bfloat16)


def more_kernel(columns, mine_ref, *refs):
    parts, (weight_ref, kept_ref, out_ref) = refs[:columns], refs[columns:]
    out_ref[...] = kept_ref[...] + project_sum(mine_ref[1], parts, weight_ref)


def layer_kernel(peers, mine_ref, *refs):
    blocks = refs[:peers]
    adj_ref, kept_ref, feat_ref, cot_ref, write_adj_ref, out_ref, grad_ref = refs[peers:peers + 7]
    partial_refs = refs[peers + 7:]
    preact = kept_ref[...]
    for i in range(peers):
        preact = preact + matmul(adj_ref[i], blocks[i][...])
    sigma = jax.nn.sigmoid(preact)
    out_ref[...] = (feat_ref[...].astype(jnp.float32) + preact * sigma).astype(jnp.bfloat16)
    slope = sigma * (1.0 + preact * (1.0 - sigma))
    grad = (cot_ref[...].astype(jnp.float32) * slope).astype(jnp.bfloat16)
    grad_ref[...] = grad
    for i in range(peers):
        partial_refs[i][...] = matmul_rows(write_adj_ref[i], grad).astype(partial_refs[i].dtype)


def back_kernel(columns, mine_ref, *refs):
    parts, (cite_ref, self_ref, adj_ref, cot_ref) = refs[:columns], refs[columns:columns + 4]
    partial_refs = refs[columns + 4:]
    mine = mine_ref[1]
    cite_grad = project_back_sum(mine, parts, cite_ref).astype(jnp.bfloat16)
    for i in range(len(partial_refs) - 1, 0, -1):
        partial_refs[i][...] = matmul_rows(adj_ref[i], cite_grad).astype(jnp.bfloat16)
    partial_refs[0][...] = (
        cot_ref[...].astype(jnp.float32)
        + project_back_sum(mine, parts, self_ref)
        + matmul_rows(adj_ref[0], cite_grad)
    )


def leave_kernel(columns, mine_ref, *refs):
    parts, (weight_ref, out_ref) = refs[:columns], refs[columns:]
    out_ref[...] = project_back_sum(mine_ref[1], parts, weight_ref).astype(jnp.bfloat16)


def body(
    paper_feat,
    author_feat,
    cite_owner,
    cite_source,
    cite_target,
    cite_edges,
    cite_count,
    citation_weight_tiles,
    write_owner,
    write_paper,
    write_author,
    write_edges,
    authorship_weight_tiles,
    w_self,
    w_cite,
    w_write,
    cotangent,
):
    peers = lax.axis_size("paper")
    columns = lax.axis_size("author")
    side = citation_weight_tiles.shape[1]
    paper_rows, quarter = paper_feat.shape
    author_rows = author_feat.shape[0]
    paper_blocks = paper_rows // side
    author_blocks = author_rows // side
    places = jnp.stack([lax.axis_index("paper"), lax.axis_index("author")])
    bf16 = jnp.bfloat16
    f32 = jnp.float32
    paper_tile = (paper_rows, quarter)
    author_tile = (author_rows, quarter)

    near = fits(peers * paper_rows, paper_rows)

    feats = feature_gather(paper_feat, columns)
    authors = ring_gather(author_feat, peers, 1)
    tables = [
        write_owner.reshape(-1), write_paper, write_author, write_edges,
        cite_owner.reshape(-1), cite_target, cite_source, cite_edges,
    ]
    windows, tables, mine = fetch(places, cite_count, [w_cite, w_self, w_write], tables, quarter, near)
    cite_window, self_window, write_window = windows
    projected, kept = run(
        functools.partial(enter_kernel, columns), mine, [*feats, cite_window, self_window],
        [(paper_tile, bf16), (paper_tile, f32)], near,
    )
    sources = ring_gather(projected, peers, -1)
    write_adj = adjacency(
        False, mine, tables[:4], authorship_weight_tiles, peers, paper_blocks, author_blocks,
        near, (projected,),
    )
    cite_adj = adjacency(
        True, mine, tables[4:], citation_weight_tiles, peers, paper_blocks, paper_blocks,
        near, (projected,),
    )
    write_sum, = run(
        functools.partial(gather_kernel, peers), mine, [*authors, write_adj],
        [(paper_tile, bf16)], near,
    )
    writes = feature_gather(write_sum, columns)
    kept, = run(
        functools.partial(more_kernel, columns), mine, [*writes, write_window, kept],
        [(paper_tile, f32)], near,
    )
    paper_out, grad_pre, *author_partials = run(
        functools.partial(layer_kernel, peers), mine,
        [*sources, cite_adj, kept, paper_feat, cotangent, write_adj],
        [(paper_tile, bf16), (paper_tile, bf16), (author_tile, f32)]
        + [(author_tile, bf16)] * (peers - 1), near, kept=(0,),
    )
    grads = feature_gather(grad_pre, columns)
    author_sum = ring_scatter(author_partials, peers, 1).astype(bf16)
    paper_partials = run(
        functools.partial(back_kernel, columns), mine,
        [*grads, w_cite, w_self, cite_adj, cotangent],
        [(paper_tile, f32)] + [(paper_tile, bf16)] * (peers - 1), near,
    )
    paper_grad = ring_scatter(paper_partials, peers, -1).astype(bf16)
    author_sums = feature_gather(author_sum, columns)
    author_grad, = run(
        functools.partial(leave_kernel, columns), mine, [*author_sums, w_write],
        [(author_tile, bf16)], near, kept=(0,),
    )
    return (paper_out, paper_grad, author_grad)


def solution(mesh):
    in_specs = (
        P("paper", "author"),
        P("paper", "author"),
        P("paper", None),
        P("paper"),
        P("paper"),
        P("paper"),
        P("paper"),
        P("paper", None, None),
        P("paper", None),
        P("paper"),
        P("paper"),
        P("paper"),
        P("paper", None, None),
        P(),
        P(),
        P(),
        P("paper", "author"),
    )
    out_specs = (P("paper", "author"), P("paper", "author"), P("paper", "author"))
    return jax.shard_map(body, mesh=mesh, in_specs=in_specs, out_specs=out_specs, check_vma=False)
```

```python
import functools
import jax
import jax.numpy as jnp
from jax import lax
from jax.experimental import pallas as pl
from jax.experimental.pallas import tpu as pltpu
from jax.sharding import PartitionSpec as P


def matmul(left, right):
    return jnp.dot(left, right, preferred_element_type=jnp.float32)


def matmul_flipped(left, right):
    return lax.dot_general(
        left, right, (((1,), (1,)), ((), ())), preferred_element_type=jnp.float32
    )


def matmul_rows(left, right):
    return lax.dot_general(
        left, right, (((0,), (0,)), ((), ())), preferred_element_type=jnp.float32
    )


def ring_order(count):
    if count % 2:
        return list(range(count))
    return list(range(0, count, 2)) + list(range(count - 1, 0, -2))


def ring_place(index, count):
    if count % 2:
        return index
    return jnp.where(index % 2 == 0, index // 2, count - (index + 1) // 2)


def ring_pairs(count, step):
    order = ring_order(count)
    return [(order[i], order[(i + step) % count]) for i in range(count)]


def ring_gather(block, count, first):
    ups = count // 2 if first > 0 else (count - 1) // 2
    blocks = {0: block}
    for reach, step in ((ups, 1), (count - 1 - ups, -1)):
        held = block
        for place in range(1, reach + 1):
            held = lax.ppermute(held, "paper", ring_pairs(count, step))
            blocks[-place * step % count] = held
    return [blocks[i] for i in range(count)]


def ring_scatter(partials, count, first):
    ups = count // 2 if first > 0 else (count - 1) // 2
    terms = [partials[0]]
    for reach, step in ((ups, 1), (count - 1 - ups, -1)):
        if reach == 0:
            continue
        held = partials[reach * step % count]
        for place in range(reach - 1, 0, -1):
            held = lax.ppermute(held, "paper", ring_pairs(count, step))
            held = held.astype(jnp.float32) + partials[place * step % count].astype(jnp.float32)
            held = held.astype(jnp.bfloat16)
        held = lax.ppermute(held, "paper", ring_pairs(count, step))
        terms.append(held)
    return terms


def feature_gather(part, count):
    parts = {0: part}
    bit = count // 2
    while bit:
        pairs = [(i, i ^ bit) for i in range(count)]
        for r, held in list(parts.items()):
            parts[r ^ bit] = lax.ppermute(held, "author", pairs)
        bit //= 2
    return [parts[r] for r in range(count)]


VMEM_ELEMENTS = 1 << 20
VMEM_GRANT = 12 << 20
SMEM = pl.BlockSpec(memory_space=pltpu.SMEM)
VMEM = pl.BlockSpec(memory_space=pltpu.VMEM)


def adjacency_kernel(peers, counted, mine_ref, owner_ref, inner_ref, outer_ref, edges_ref, tiles_ref, *refs):
    out_ref, acc_ref = refs[-2:]
    groups, rows, cols = out_ref.shape
    side = tiles_ref.shape[1]
    across = cols // side
    down = rows // side
    here = ring_place(mine_ref[0], peers)
    limit = mine_ref[2] if counted else tiles_ref.shape[0]
    acc_ref[...] = jnp.zeros(acc_ref.shape, jnp.float32)

    def add(tile, carry):
        group = lax.rem(ring_place(owner_ref[tile], peers) - here + peers, peers)
        place = (group * down + inner_ref[tile]) * across + outer_ref[tile]
        edges = jnp.full((1, side), edges_ref[tile].astype(jnp.float32))
        live = jnp.where(tile < limit, 1.0, 0.0)
        acc_ref[place] += (live / edges) * tiles_ref[tile].astype(jnp.float32)
        return carry

    lax.fori_loop(0, tiles_ref.shape[0], add, 0, unroll=8)

    def store(group, carry):
        for i in range(down):
            for j in range(across):
                out_ref[group, i * side:(i + 1) * side, j * side:(j + 1) * side] = acc_ref[
                    (group * down + i) * across + j
                ].astype(jnp.bfloat16)
        return carry

    lax.fori_loop(0, groups, store, 0)


def adjacency(counted, mine, tables, tiles, peers, down, across, near, after):
    side = tiles.shape[1]
    call = pl.pallas_call(
        functools.partial(adjacency_kernel, peers, counted),
        out_shape=(pltpu.VMEM if near else jax.ShapeDtypeStruct)(
            (peers, down * side, across * side), jnp.bfloat16
        ),
        in_specs=[SMEM] * 5 + [VMEM] * (1 + len(after)),
        out_specs=VMEM,
        compiler_params=grant(near),
        scratch_shapes=[pltpu.VMEM((peers * down * across, side, side), jnp.float32)],
    )
    return call(
        mine, *tables, placed(tiles, near), *[placed(v, near) for v in after]
    )


def project_sum(mine, parts, weight_ref):
    quarter = parts[0].shape[1]
    total = None
    for r, part in enumerate(parts):
        start = pl.multiple_of((mine ^ r) * quarter, quarter)
        piece = matmul(part[...], weight_ref[pl.ds(start, quarter), :])
        total = piece if total is None else total + piece
    return total


def project_back_sum(mine, parts, weight_ref):
    quarter = parts[0].shape[1]
    own = pl.multiple_of(mine * quarter, quarter)
    total = None
    for r, part in enumerate(parts):
        start = pl.multiple_of((mine ^ r) * quarter, quarter)
        piece = matmul_flipped(part[...], weight_ref[pl.ds(own, quarter), pl.ds(start, quarter)])
        total = piece if total is None else total + piece
    return total


def fits(rows, cols):
    return rows * cols <= VMEM_ELEMENTS


def grant(near):
    return pltpu.CompilerParams(vmem_limit_bytes=VMEM_GRANT) if near else None


def placed(array, near):
    return pltpu.with_memory_space_constraint(array, pltpu.VMEM) if near else array


def run(kernel, mine, inputs, outs, near, after=(), kept=()):
    return pl.pallas_call(
        kernel,
        in_specs=[SMEM] + [VMEM] * (len(inputs) + len(after)),
        out_specs=[VMEM] * len(outs),
        out_shape=[
            (pltpu.VMEM if near and i not in kept else jax.ShapeDtypeStruct)(shape, dtype)
            for i, (shape, dtype) in enumerate(outs)
        ],
        compiler_params=grant(near),
    )(mine, *[placed(v, near) for v in inputs], *[placed(v, near) for v in after])


def fetch_kernel(weight_count, place_ref, count_ref, *refs):
    scalars_ref, sems = refs[-2:]
    refs = refs[:-2]
    sources, targets = refs[:len(refs) // 2], refs[len(refs) // 2:]
    quarter = targets[0].shape[1]
    own = pl.multiple_of(place_ref[1] * quarter, quarter)
    copies = []
    for i, (source, target) in enumerate(zip(sources, targets)):
        if i < weight_count:
            source = source.at[:, pl.ds(own, quarter)]
        copies.append(pltpu.make_async_copy(source, target, sems.at[i]))
    for copy in copies:
        copy.start()
    scalars_ref[0] = place_ref[0]
    scalars_ref[1] = place_ref[1]
    scalars_ref[2] = count_ref[0]
    for copy in copies:
        copy.wait()


def fetch(places, live, weights, tables, quarter, near):
    space = pltpu.VMEM if near else jax.ShapeDtypeStruct
    sources = [pltpu.with_memory_space_constraint(v, pltpu.HBM) for v in [*weights, *tables]]
    call = pl.pallas_call(
        functools.partial(fetch_kernel, len(weights)),
        in_specs=[SMEM, SMEM] + [pl.BlockSpec(memory_space=pltpu.HBM)] * len(sources),
        out_specs=[VMEM] * len(weights) + [SMEM] * (len(tables) + 1),
        out_shape=[space((weight.shape[0], quarter), weight.dtype) for weight in weights]
        + [pltpu.SMEM(table.shape, jnp.int32) for table in tables]
        + [pltpu.SMEM((3,), jnp.int32)],
        scratch_shapes=[pltpu.SemaphoreType.DMA((len(sources),))],
        compiler_params=grant(near),
    )
    *found, scalars = call(places, live, *sources)
    return found[:len(weights)], found[len(weights):], scalars


def enter_kernel(columns, mine_ref, *refs):
    parts, (cite_ref, self_ref) = refs[:columns], refs[columns:columns + 2]
    projected_ref, kept_ref = refs[-2:]
    mine = mine_ref[1]
    projected_ref[...] = project_sum(mine, parts, cite_ref).astype(jnp.bfloat16)
    kept_ref[...] = project_sum(mine, parts, self_ref)


def gather_kernel(peers, mine_ref, *refs):
    blocks, adj_ref, out_ref = refs[:peers], refs[peers], refs[-1]
    total = matmul(adj_ref[0], blocks[0][...])
    for i in range(1, peers):
        total = total + matmul(adj_ref[i], blocks[i][...])
    out_ref[...] = total.astype(jnp.bfloat16)


def more_kernel(columns, mine_ref, *refs):
    parts, (weight_ref, kept_ref, out_ref) = refs[:columns], refs[columns:]
    out_ref[...] = kept_ref[...] + project_sum(mine_ref[1], parts, weight_ref)


def layer_kernel(peers, mine_ref, *refs):
    blocks = refs[:peers]
    adj_ref, kept_ref, feat_ref, cot_ref, out_ref, grad_ref = refs[peers:]
    preact = kept_ref[...]
    for i in range(peers):
        preact = preact + matmul(adj_ref[i], blocks[i][...])
    sigma = jax.nn.sigmoid(preact)
    out_ref[...] = (feat_ref[...].astype(jnp.float32) + preact * sigma).astype(jnp.bfloat16)
    slope = sigma * (1.0 + preact * (1.0 - sigma))
    grad = (cot_ref[...].astype(jnp.float32) * slope).astype(jnp.bfloat16)
    grad_ref[...] = grad


def share_kernel(peers, mine_ref, grad_ref, adj_ref, *partial_refs):
    grad = grad_ref[...]
    for i in range(peers - 1, -1, -1):
        partial_refs[i][...] = matmul_rows(adj_ref[i], grad).astype(partial_refs[i].dtype)


def back_kernel(columns, mine_ref, *refs):
    parts, (cite_ref, self_ref, adj_ref, cot_ref) = refs[:columns], refs[columns:columns + 4]
    partial_refs = refs[columns + 4:]
    mine = mine_ref[1]
    cite_grad = project_back_sum(mine, parts, cite_ref).astype(jnp.bfloat16)
    for i in range(len(partial_refs) - 1, 0, -1):
        partial_refs[i][...] = matmul_rows(adj_ref[i], cite_grad).astype(jnp.bfloat16)
    partial_refs[0][...] = (
        cot_ref[...].astype(jnp.float32)
        + project_back_sum(mine, parts, self_ref)
        + matmul_rows(adj_ref[0], cite_grad)
    )


def leave_kernel(columns, mine_ref, *refs):
    parts, (weight_ref, kept_ref, *terms) = refs[:columns], refs[columns:-3]
    out_ref, paper_ref, author_ref = refs[-3:]
    out_ref[...] = kept_ref[...]
    total = terms[0][...]
    for term in terms[1:]:
        total = total + term[...].astype(jnp.float32)
    paper_ref[...] = total.astype(jnp.bfloat16)
    author_ref[...] = project_back_sum(mine_ref[1], parts, weight_ref).astype(jnp.bfloat16)


def body(
    paper_feat,
    author_feat,
    cite_owner,
    cite_source,
    cite_target,
    cite_edges,
    cite_count,
    citation_weight_tiles,
    write_owner,
    write_paper,
    write_author,
    write_edges,
    authorship_weight_tiles,
    w_self,
    w_cite,
    w_write,
    cotangent,
):
    peers = lax.axis_size("paper")
    columns = lax.axis_size("author")
    side = citation_weight_tiles.shape[1]
    paper_rows, quarter = paper_feat.shape
    author_rows = author_feat.shape[0]
    paper_blocks = paper_rows // side
    author_blocks = author_rows // side
    places = jnp.stack([lax.axis_index("paper"), lax.axis_index("author")])
    bf16 = jnp.bfloat16
    f32 = jnp.float32
    paper_tile = (paper_rows, quarter)
    author_tile = (author_rows, quarter)

    near = fits(peers * paper_rows, paper_rows)

    feats = feature_gather(paper_feat, columns)
    authors = ring_gather(author_feat, peers, 1)
    tables = [
        write_owner.reshape(-1), write_paper, write_author, write_edges,
        cite_owner.reshape(-1), cite_target, cite_source, cite_edges,
    ]
    windows, tables, mine = fetch(places, cite_count, [w_cite, w_self, w_write], tables, quarter, near)
    cite_window, self_window, write_window = windows
    projected, kept = run(
        functools.partial(enter_kernel, columns), mine, [*feats, cite_window, self_window],
        [(paper_tile, bf16), (paper_tile, f32)], near,
    )
    sources = ring_gather(projected, peers, -1)
    write_adj = adjacency(
        False, mine, tables[:4], authorship_weight_tiles, peers, paper_blocks, author_blocks,
        near, (projected,),
    )
    cite_adj = adjacency(
        True, mine, tables[4:], citation_weight_tiles, peers, paper_blocks, paper_blocks,
        near, (projected,),
    )
    write_sum, = run(
        functools.partial(gather_kernel, peers), mine, [*authors, write_adj],
        [(paper_tile, bf16)], near,
    )
    writes = feature_gather(write_sum, columns)
    kept, = run(
        functools.partial(more_kernel, columns), mine, [*writes, write_window, kept],
        [(paper_tile, f32)], near,
    )
    paper_out, grad_pre = run(
        functools.partial(layer_kernel, peers), mine,
        [*sources, cite_adj, kept, paper_feat, cotangent], [(paper_tile, bf16), (paper_tile, bf16)], near,
    )
    author_partials = run(
        functools.partial(share_kernel, peers), mine, [grad_pre, write_adj],
        [(author_tile, f32)] + [(author_tile, bf16)] * (peers - 1), near,
    )
    grads = feature_gather(grad_pre, columns)
    author_terms = ring_scatter(author_partials, peers, 1)
    author_sum = sum(term.astype(f32) for term in author_terms).astype(bf16)
    paper_partials = run(
        functools.partial(back_kernel, columns), mine,
        [*grads, w_cite, w_self, cite_adj, cotangent],
        [(paper_tile, f32)] + [(paper_tile, bf16)] * (peers - 1), near,
    )
    paper_terms = ring_scatter(paper_partials, peers, -1)
    author_sums = feature_gather(author_sum, columns)
    paper_out, paper_grad, author_grad = run(
        functools.partial(leave_kernel, columns), mine,
        [*author_sums, w_write, paper_out, *paper_terms],
        [(paper_tile, bf16), (paper_tile, bf16), (author_tile, bf16)], near, kept=(0, 1, 2),
    )
    return (paper_out, paper_grad, author_grad)


def solution(mesh):
    in_specs = (
        P("paper", "author"),
        P("paper", "author"),
        P("paper", None),
        P("paper"),
        P("paper"),
        P("paper"),
        P("paper"),
        P("paper", None, None),
        P("paper", None),
        P("paper"),
        P("paper"),
        P("paper"),
        P("paper", None, None),
        P(),
        P(),
        P(),
        P("paper", "author"),
    )
    out_specs = (P("paper", "author"), P("paper", "author"), P("paper", "author"))
    return jax.shard_map(body, mesh=mesh, in_specs=in_specs, out_specs=out_specs, check_vma=False)
```
